8 devices in a mesh: sys: 1 (over z), seg: 8 (over y, x, core).
Axes of the slice: x: 2, y: 2, z: 1, core: 2. Of those that a mesh axis runs over, the one named last changes fastest.
Arguments:
- positions: bfloat16 [16384, 320], P(('sys', 'seg'))
- charges: float32 [16384], P(('sys', 'seg'))
- pair_band: int32 [8, 7], P(('sys', 'seg'))
Outputs:
- output 1: float32 [16384, 320], P(('sys', 'seg'))
- output 2: float32 [1], P('sys')
All inputs are finite; a program needn't handle non-finite values.
Results may differ from the reference program's by a relative error of at most 0.001.
Values are sent between devices in bfloat16 or wider.
A program may use at most 1 GiB of HBM per device.

```python
import jax
import jax.numpy as jnp
from jax import lax

SEG_COUNT = 8
BLOCK_ROWS = 2048
FEAT_DIM = 320
REACH_STEPS = 3


def draw_band(mask_key):
    coin_draw = jax.random.randint(mask_key, (SEG_COUNT, REACH_STEPS), 0, 3)
    block_ids = jnp.arange(SEG_COUNT)[:, None]
    step_ids = jnp.arange(REACH_STEPS)[None, :]
    upper_cols = jnp.where((block_ids == 0) & (step_ids == REACH_STEPS - 1), 1, (coin_draw > 0).astype(jnp.int32))
    lower_list = [jnp.roll(upper_cols[:, step_idx - 1], step_idx) for step_idx in range(REACH_STEPS, 0, -1)]
    higher_list = [upper_cols[:, step_idx - 1] for step_idx in range(1, REACH_STEPS + 1)]
    centre_list = [jnp.ones((SEG_COUNT,), jnp.int32)]
    return jnp.stack(lower_list + centre_list + higher_list, axis=1).astype(jnp.int32)


def setup_inputs(seed: int = 0, part: int = 0) -> dict:
    part_key = jax.random.fold_in(jax.random.key(seed), part)
    pos_key, sign_key, mag_key, mask_key = jax.random.split(part_key, 4)
    all_rows = SEG_COUNT * BLOCK_ROWS
    pos_vals = jax.random.normal(pos_key, (all_rows, FEAT_DIM), jnp.float32)
    sign_vals = 2.0 * jax.random.randint(sign_key, (all_rows,), 0, 2).astype(jnp.float32) - 1.0
    magnitude = jax.random.uniform(mag_key, (all_rows,), jnp.float32, 0.5, 1.5)
    charge_scale = FEAT_DIM ** 0.5 * (BLOCK_ROWS * (2 * REACH_STEPS + 1)) ** -0.25
    return {'positions': pos_vals.astype(jnp.bfloat16), 'charges': sign_vals * magnitude * charge_scale, 'pair_band': draw_band(mask_key)}


def reference(positions, charges, pair_band):
    inv_lsq = 1.0 / FEAT_DIM
    pos_blocks = positions.reshape(SEG_COUNT, BLOCK_ROWS, FEAT_DIM)
    charge_blocks = charges.reshape(SEG_COUNT, BLOCK_ROWS)
    row_ids = jnp.arange(BLOCK_ROWS)
    self_pair = row_ids[:, None] == row_ids[None, :]
    offsets = jnp.arange(-REACH_STEPS, REACH_STEPS + 1)

    def one_block(host_blk):
        x_host = pos_blocks[host_blk]
        host_f32 = x_host.astype(jnp.float32)
        host_sq = jnp.sum(host_f32 * host_f32, axis=1)
        q_host = charge_blocks[host_blk]

        def one_offset(carry_state, offset):
            force_acc, energy_acc = carry_state
            other_blk = (host_blk + offset) % SEG_COUNT
            x_other = pos_blocks[other_blk]
            other_f32 = x_other.astype(jnp.float32)
            other_sq = jnp.sum(other_f32 * other_f32, axis=1)
            cross_dot = jnp.dot(x_host, x_other.T, preferred_element_type=jnp.float32)
            sq_dist = jnp.maximum(host_sq[:, None] + other_sq[None, :] - 2.0 * cross_dot, 0.0)
            weights = q_host[:, None] * charge_blocks[other_blk][None, :] * jnp.exp(sq_dist * (-0.5 * inv_lsq))
            keep_pair = (pair_band[host_blk, REACH_STEPS + offset] != 0) & jnp.logical_not(self_pair & (offset == 0))
            weights = jnp.where(keep_pair, weights, 0.0)
            pull_term = jnp.dot(weights.astype(jnp.bfloat16), x_other, preferred_element_type=jnp.float32)
            force_acc = force_acc + (jnp.sum(weights, axis=1)[:, None] * host_f32 - pull_term) * inv_lsq
            energy_acc = energy_acc + 0.5 * jnp.sum(weights)
            return (force_acc, energy_acc), None

        init_carry = (jnp.zeros((BLOCK_ROWS, FEAT_DIM), jnp.float32), jnp.zeros((), jnp.float32))
        (force_blk, energy_blk), _ = lax.scan(one_offset, init_carry, offsets)
        return force_blk, energy_blk

    force_blocks, block_energy = lax.map(one_block, jnp.arange(SEG_COUNT))
    return force_blocks.reshape(SEG_COUNT * BLOCK_ROWS, FEAT_DIM), jnp.sum(block_energy).reshape(1)
```

```python
import functools

import jax
import jax.numpy as jnp
from jax import lax
from jax.experimental import pallas as pl
from jax.experimental.pallas import tpu as pltpu
from jax.sharding import PartitionSpec as P

MESH = pl.DeviceIdType.MESH
LOG2E = 1.4426950408889634
CHUNK = 512
TILE = 256
PARTS = 4
ORDER = [(0, c) for c in range(4)] + [(1, c) for c in range(4)] + [
    (2, 0), (4, 0), (3, 0), (2, 1), (4, 1), (3, 1), (2, 2), (4, 2), (3, 2), (2, 3), (4, 3), (3, 3),
    (6, 0), (5, 2), (5, 0), (6, 2), (6, 1), (5, 3), (5, 1), (6, 3)]
POS = {rc: i for i, rc in enumerate(ORDER)}
N_CHUNK = len(ORDER)
FORWARDS = (
    [((2, c), 'core', (3, c)) for c in range(4)]
    + [((4, c), 'x', (6, c)) for c in range(2)]
    + [((2, c), 'y', (5, c)) for c in range(2, 4)]
    + [((6, c), 'core', (5, c)) for c in range(2)]
    + [((5, c), 'core', (6, c)) for c in range(2, 4)])
FIRSTS = [((0, c), link, (role, c)) for c in range(4) for link, role in (('x', 2), ('yo', 4), ('core', 1))]
SENDS = FIRSTS + FORWARDS


def split3(v):
    hi = v.astype(jnp.bfloat16)
    rest = v - hi.astype(jnp.float32)
    mid = rest.astype(jnp.bfloat16)
    low = (rest - mid.astype(jnp.float32)).astype(jnp.bfloat16)
    return hi.astype(jnp.float32), mid.astype(jnp.float32), low.astype(jnp.float32)


def kernel(inv_lsq, x_ref, q_ref, band_ref, out_ref, en_ref,
           xi, xj, qj, qi, s0, s1, acc, rs, bound, eslot, mpos,
           send_x, recv_x, send_q, recv_q, send_e, recv_e):
    n_rows, feat = x_ref.shape
    depth = xj.shape[1]
    n_tiles = n_rows // TILE
    scale = LOG2E * inv_lsq
    my_sys = lax.axis_index('sys')
    me = lax.axis_index('seg')
    core = lax.rem(me, 2)
    xc = lax.rem(me // 2, 2)
    yc = me // 4

    def dev(y, x, c):
        return (y * 2 + x) * 2 + c

    owner = {0: me, 1: dev(yc, xc, 1 - core), 2: dev(yc, 1 - xc, core), 3: dev(yc, 1 - xc, 1 - core),
             4: dev(1 - yc, xc, 1 - core), 5: dev(1 - yc, 1 - xc, core), 6: dev(1 - yc, 1 - xc, 1 - core)}
    target = {'core': owner[1], 'x': owner[2], 'yo': owner[4], 'y': dev(1 - yc, xc, core)}

    barrier = pltpu.get_barrier_semaphore()
    for step in range(1, 8):
        pl.semaphore_signal(barrier, inc=1, device_id=(my_sys, lax.rem(me + step, 8)), device_id_type=MESH)

    def copies(k):
        src, link, dst = SENDS[k]
        s, d = POS[src], POS[dst]
        to = (my_sys, target[link])
        return (
            pltpu.make_async_remote_copy(src_ref=qj.at[s], dst_ref=qj.at[d], send_sem=send_q.at[k],
                                         recv_sem=recv_q.at[d], device_id=to, device_id_type=MESH),
            pltpu.make_async_remote_copy(src_ref=xj.at[s], dst_ref=xj.at[d], send_sem=send_x.at[k],
                                         recv_sem=recv_x.at[d], device_id=to, device_id_type=MESH))

    def arrived(p):
        to = (my_sys, me)
        pltpu.make_async_remote_copy(src_ref=qj.at[p], dst_ref=qj.at[p], send_sem=send_q.at[0],
                                     recv_sem=recv_q.at[p], device_id=to, device_id_type=MESH).wait_recv()
        pltpu.make_async_remote_copy(src_ref=xj.at[p], dst_ref=xj.at[p], send_sem=send_x.at[0],
                                     recv_sem=recv_x.at[p], device_id=to, device_id_type=MESH).wait_recv()

    lane = lax.broadcasted_iota(jnp.int32, (128, 128), 1)
    for g in range(n_rows // 128):
        r0 = g * 128
        c, j0 = r0 // CHUNK, r0 % CHUNK
        rows = slice(r0, r0 + 128)
        x_a = x_ref[rows, 0:128]
        x_b = x_ref[rows, 128:256]
        xi[rows, 0:128] = x_a
        xi[rows, 128:256] = x_b
        xi[rows, 256:feat] = x_ref[rows, 256:feat]
        x_c = xi[rows, 256:384].astype(jnp.float32)
        x_c = jnp.where(lane < feat - 256, x_c, 0.0)
        fa, fb = x_a.astype(jnp.float32), x_b.astype(jnp.float32)
        half = -0.5 * jnp.sum(fa * fa + fb * fb + x_c * x_c, axis=1, keepdims=True)
        pieces = split3(half)
        l0 = feat - 256
        v_i = jnp.where((lane >= l0) & (lane < l0 + 3), 1.0, x_c)
        v_j = jnp.where((lane >= l0 + 3) & (lane < l0 + 6), 1.0, x_c)
        for k in range(3):
            v_i = jnp.where(lane == l0 + 3 + k, pieces[k], v_i)
            v_j = jnp.where(lane == l0 + k, pieces[k], v_j)
        xi[rows, 256:384] = v_i.astype(jnp.bfloat16)
        xj[c, 0:128, j0:j0 + 128] = x_a.T
        xj[c, 128:256, j0:j0 + 128] = x_b.T
        xj[c, 256:depth, j0:j0 + 128] = v_j.T[0:depth - 256].astype(jnp.bfloat16)
        q_row = q_ref[:, rows]
        qj[c, :, j0:j0 + 128] = q_row
        qi[rows, :] = jnp.broadcast_to(q_row, (128, 128)).T

    pl.semaphore_wait(barrier, 7)
    for k in range(len(FIRSTS)):
        for copy in copies(k):
            copy.start()

    tr = lax.broadcasted_iota(jnp.int32, (TILE, TILE), 0)
    tc = lax.broadcasted_iota(jnp.int32, (TILE, TILE), 1)
    bound[0] = jnp.zeros((TILE, TILE), jnp.float32)
    bound[1] = jnp.where(tr == tc, -1e30, 0.0)
    acc[...] = jnp.zeros_like(acc)
    rs[...] = jnp.zeros_like(rs)
    for p, (role, _) in enumerate(ORDER):
        mpos[p] = band_ref[0, lax.rem(owner[role] - me + 11, 8)].astype(jnp.float32)

    def cross(p, t, jt, s_new):
        rows, cols = slice(t * TILE, (t + 1) * TILE), slice(jt * TILE, (jt + 1) * TILE)
        s_new[jt, rows, :] = jnp.dot(xi[rows, 0:depth], xj[p, :, cols], preferred_element_type=jnp.float32)

    def phase(p_new, s_new, p_old, s_old):
        mark = None if p_old is None else mpos[p_old]
        for t in range(n_tiles):
            rows = slice(t * TILE, (t + 1) * TILE)
            row_part, pull = None, None
            for jt in range(CHUNK // TILE):
                cols = slice(jt * TILE, (jt + 1) * TILE)
                if s_new is not None:
                    cross(p_new, t, jt, s_new)
                s = s_old[jt, rows, :]
                if t % 2 == jt:
                    top = bound[jnp.where(p_old == t // 2, 1, 0)]
                else:
                    top = 0.0
                e = jnp.exp2(jnp.minimum(s, top) * scale)
                q_rows = qi[rows, :]
                w = jnp.concatenate([e[:, 0:128] * q_rows, e[:, 128:256] * q_rows], axis=1)
                w = w * (qj[p_old, :, cols] * mark)
                part = w[:, 0:128] + w[:, 128:256]
                row_part = part if row_part is None else row_part + part
                prod = lax.dot_general(xj[p_old, 0:feat, cols], w.astype(jnp.bfloat16), (((1,), (1,)), ((), ())),
                                       preferred_element_type=jnp.float32)
                pull = prod if pull is None else pull + prod
            acc[:, rows] += pull
            rs[rows, :] += row_part

    for t in range(n_tiles):
        for jt in range(CHUNK // TILE):
            cross(0, t, jt, s1)

    def pass_on(p):
        for k in range(len(FIRSTS), len(SENDS)):
            if POS[SENDS[k][0]] == p:
                for copy in copies(k):
                    copy.start()

    forward_at = sorted({POS[f[0]] for f in FORWARDS})

    def pair(i, carry):
        p1, p2 = 2 * i + 1, 2 * i + 2

        @pl.when(p1 >= PARTS)
        def _():
            arrived(p1)

        @pl.when(p2 >= PARTS)
        def _():
            arrived(p2)

        for f in sorted({(fp - 1) // 2 for fp in forward_at}):
            @pl.when(i == f)
            def _():
                for fp in forward_at:
                    if (fp - 1) // 2 == f:
                        pass_on(fp)

        phase(p1, s0, p1 - 1, s1)
        phase(p2, s1, p1, s0)
        return carry

    lax.fori_loop(0, (N_CHUNK - 2) // 2, pair, 0)
    arrived(N_CHUNK - 1)
    phase(N_CHUNK - 1, s0, N_CHUNK - 2, s1)
    phase(None, None, N_CHUNK - 1, s0)

    eslot[me] = 0.5 * jnp.sum(rs[...].reshape(n_rows // 8, 8, 128), axis=0)

    def finish(g):
        rows = slice(g * 128, (g + 1) * 128)
        total = jnp.sum(rs[rows, :], axis=1, keepdims=True)
        for k0, k1 in ((0, 128), (128, 256), (256, feat)):
            x_part = x_ref[rows, k0:k1].astype(jnp.float32)
            out_ref[rows, k0:k1] = (total * x_part - acc[k0:k1, rows].T) * inv_lsq

    def energy_copy(step):
        return pltpu.make_async_remote_copy(
            src_ref=eslot.at[me], dst_ref=eslot.at[me], send_sem=send_e.at[step - 1],
            recv_sem=recv_e.at[step - 1], device_id=(my_sys, lax.rem(me + step, 8)), device_id_type=MESH)

    for g in range(n_rows // 256):
        finish(g)
    for step in range(1, 8):
        energy_copy(step).start()
    for g in range(n_rows // 256, n_rows // 128):
        finish(g)
    for k in range(len(SENDS)):
        for copy in copies(k):
            copy.wait_send()
    for step in range(1, 8):
        energy_copy(step).wait_send()
        src = lax.rem(me - step + 8, 8)
        pltpu.make_async_remote_copy(
            src_ref=eslot.at[src], dst_ref=eslot.at[src], send_sem=send_e.at[step - 1],
            recv_sem=recv_e.at[step - 1], device_id=(my_sys, me), device_id_type=MESH).wait_recv()
    total = eslot[0]
    for d in range(1, 8):
        total = total + eslot[d]
    en_ref[...] = jnp.broadcast_to(jnp.sum(total, keepdims=True), en_ref.shape)


def solution(mesh):
    def device_fn(positions, charges, pair_band):
        n_rows, feat = positions.shape
        depth = feat + 16
        vmem = pl.BlockSpec(memory_space=pltpu.VMEM)
        f32, bf16 = jnp.float32, jnp.bfloat16
        dma = pltpu.SemaphoreType.DMA
        forces, energy = pl.pallas_call(
            functools.partial(kernel, 1.0 / feat),
            out_shape=[jax.ShapeDtypeStruct((n_rows, feat), f32), jax.ShapeDtypeStruct((8, 128), f32)],
            in_specs=[vmem, vmem, pl.BlockSpec(memory_space=pltpu.SMEM)],
            out_specs=[vmem, vmem],
            scratch_shapes=[
                pltpu.VMEM((n_rows, 384), bf16),
                pltpu.VMEM((N_CHUNK, depth, CHUNK), bf16),
                pltpu.VMEM((N_CHUNK, 1, CHUNK), f32),
                pltpu.VMEM((n_rows, 128), f32),
                pltpu.VMEM((CHUNK // TILE, n_rows, TILE), f32),
                pltpu.VMEM((CHUNK // TILE, n_rows, TILE), f32),
                pltpu.VMEM((feat, n_rows), f32),
                pltpu.VMEM((n_rows, 128), f32),
                pltpu.VMEM((2, TILE, TILE), f32),
                pltpu.VMEM((8, 8, 128), f32),
                pltpu.SMEM((N_CHUNK,), f32),
                dma((len(SENDS),)), dma((N_CHUNK,)), dma((len(SENDS),)), dma((N_CHUNK,)),
                dma((7,)), dma((7,)),
            ],
            compiler_params=pltpu.CompilerParams(
                collective_id=0, has_side_effects=True, vmem_limit_bytes=60 * 1024 * 1024),
            name='pair_forces',
        )(positions, charges.reshape(1, n_rows), pair_band)
        return forces, energy[0, 0:1]

    row_spec = P(('sys', 'seg'), None)
    vec_spec = P(('sys', 'seg'))
    return jax.shard_map(device_fn, mesh=mesh, in_specs=(row_spec, vec_spec, row_spec),
                         out_specs=(row_spec, P('sys')), check_vma=False)
```

```python
import functools

import jax
import jax.numpy as jnp
from jax import lax
from jax.experimental import pallas as pl
from jax.experimental.pallas import tpu as pltpu
from jax.sharding import PartitionSpec as P

MESH = pl.DeviceIdType.MESH
LOG2E = 1.4426950408889634
CHUNK = 512
TILE = 256
PARTS = 4
ORDER = [(0, c) for c in range(4)] + [(1, c) for c in range(4)] + [
    (2, 0), (4, 0), (3, 0), (2, 1), (4, 1), (3, 1), (2, 2), (4, 2), (3, 2), (2, 3), (4, 3), (3, 3),
    (6, 0), (5, 2), (5, 0), (6, 2), (6, 1), (5, 3), (5, 1), (6, 3)]
POS = {rc: i for i, rc in enumerate(ORDER)}
N_CHUNK = len(ORDER)
FORWARDS = (
    [((2, c), 'core', (3, c)) for c in range(4)]
    + [((4, c), 'x', (6, c)) for c in range(2)]
    + [((2, c), 'y', (5, c)) for c in range(2, 4)]
    + [((6, c), 'core', (5, c)) for c in range(2)]
    + [((5, c), 'core', (6, c)) for c in range(2, 4)])
FIRSTS = [((0, c), link, (role, c)) for c in range(4) for link, role in (('x', 2), ('yo', 4), ('core', 1))]
SENDS = FIRSTS + FORWARDS


def split3(v):
    hi = v.astype(jnp.bfloat16)
    rest = v - hi.astype(jnp.float32)
    mid = rest.astype(jnp.bfloat16)
    low = (rest - mid.astype(jnp.float32)).astype(jnp.bfloat16)
    return hi.astype(jnp.float32), mid.astype(jnp.float32), low.astype(jnp.float32)


def kernel(inv_lsq, x_ref, q_ref, band_ref, out_ref, en_ref,
           xi, xj, qj, qi, s0, s1, acc, rs, bound, eslot, mpos, aux,
           send_x, recv_x, send_q, recv_q, send_e, recv_e, out_sem):
    feat, n_rows = x_ref.shape
    depth = xj.shape[1]
    n_tiles = n_rows // TILE
    scale = LOG2E * inv_lsq
    my_sys = lax.axis_index('sys')
    me = lax.axis_index('seg')
    core = lax.rem(me, 2)
    xc = lax.rem(me // 2, 2)
    yc = me // 4

    def dev(y, x, c):
        return (y * 2 + x) * 2 + c

    owner = {0: me, 1: dev(yc, xc, 1 - core), 2: dev(yc, 1 - xc, core), 3: dev(yc, 1 - xc, 1 - core),
             4: dev(1 - yc, xc, 1 - core), 5: dev(1 - yc, 1 - xc, core), 6: dev(1 - yc, 1 - xc, 1 - core)}
    target = {'core': owner[1], 'x': owner[2], 'yo': owner[4], 'y': dev(1 - yc, xc, core)}

    barrier = pltpu.get_barrier_semaphore()
    for step in range(1, 8):
        pl.semaphore_signal(barrier, inc=1, device_id=(my_sys, lax.rem(me + step, 8)), device_id_type=MESH)

    def copies(k):
        src, link, dst = SENDS[k]
        s, d = POS[src], POS[dst]
        to = (my_sys, target[link])
        return (
            pltpu.make_async_remote_copy(src_ref=qj.at[s], dst_ref=qj.at[d], send_sem=send_q.at[k],
                                         recv_sem=recv_q.at[d], device_id=to, device_id_type=MESH),
            pltpu.make_async_remote_copy(src_ref=xj.at[s], dst_ref=xj.at[d], send_sem=send_x.at[k],
                                         recv_sem=recv_x.at[d], device_id=to, device_id_type=MESH))

    def arrived(p):
        to = (my_sys, me)
        pltpu.make_async_remote_copy(src_ref=qj.at[p], dst_ref=qj.at[p], send_sem=send_q.at[0],
                                     recv_sem=recv_q.at[p], device_id=to, device_id_type=MESH).wait_recv()
        pltpu.make_async_remote_copy(src_ref=xj.at[p], dst_ref=xj.at[p], send_sem=send_x.at[0],
                                     recv_sem=recv_x.at[p], device_id=to, device_id_type=MESH).wait_recv()

    row8 = lax.broadcasted_iota(jnp.int32, (8, CHUNK), 0)
    extra_i = []
    for c in range(PARTS):
        cols = slice(c * CHUNK, (c + 1) * CHUNK)
        x_c = x_ref[:, cols]
        xj[c, 0:feat, :] = x_c
        x_f = x_c.astype(jnp.float32)
        pieces = split3(-0.5 * jnp.sum(x_f * x_f, axis=0, keepdims=True))
        v_j = jnp.where((row8 >= 3) & (row8 < 6), 1.0, 0.0)
        v_i = jnp.where(row8 < 3, 1.0, 0.0)
        for k in range(3):
            v_j = jnp.where(row8 == k, pieces[k], v_j)
            v_i = jnp.where(row8 == 3 + k, pieces[k], v_i)
        xj[c, feat:depth, :] = v_j.astype(jnp.bfloat16)
        aux[:, cols] = v_i
        qj[c] = q_ref[:, cols]

    pl.semaphore_wait(barrier, 7)
    for k in range(len(FIRSTS)):
        for copy in copies(k):
            copy.start()

    for g in range(n_rows // 128):
        rows = slice(g * 128, (g + 1) * 128)
        xi[rows, 0:128] = x_ref[0:128, rows].T
        xi[rows, 128:256] = x_ref[128:256, rows].T
        last = jnp.concatenate([x_ref[256:feat, rows].astype(jnp.float32), aux[:, rows],
                                jnp.zeros((384 - depth, 128), jnp.float32)], axis=0)
        xi[rows, 256:384] = last.T.astype(jnp.bfloat16)
        qi[rows, :] = jnp.broadcast_to(q_ref[:, rows], (128, 128)).T

    tr = lax.broadcasted_iota(jnp.int32, (TILE, TILE), 0)
    tc = lax.broadcasted_iota(jnp.int32, (TILE, TILE), 1)
    bound[0] = jnp.zeros((TILE, TILE), jnp.float32)
    bound[1] = jnp.where(tr == tc, -1e30, 0.0)
    acc[...] = jnp.zeros_like(acc)
    rs[...] = jnp.zeros_like(rs)
    for p, (role, _) in enumerate(ORDER):
        mpos[p] = band_ref[0, lax.rem(owner[role] - me + 11, 8)].astype(jnp.float32)

    def cross(p, t, jt, s_new):
        rows, cols = slice(t * TILE, (t + 1) * TILE), slice(jt * TILE, (jt + 1) * TILE)
        s_new[jt, rows, :] = jnp.dot(xi[rows, 0:depth], xj[p, :, cols], preferred_element_type=jnp.float32)

    def phase(p_new, s_new, p_old, s_old):
        mark = None if p_old is None else mpos[p_old]
        for t in range(n_tiles):
            rows = slice(t * TILE, (t + 1) * TILE)
            row_part, pull = None, None
            for jt in range(CHUNK // TILE):
                cols = slice(jt * TILE, (jt + 1) * TILE)
                if s_new is not None:
                    cross(p_new, t, jt, s_new)
                s = s_old[jt, rows, :]
                if t % 2 == jt:
                    top = bound[jnp.where(p_old == t // 2, 1, 0)]
                else:
                    top = 0.0
                e = jnp.exp2(jnp.minimum(s, top) * scale)
                q_rows = qi[rows, :]
                w = jnp.concatenate([e[:, 0:128] * q_rows, e[:, 128:256] * q_rows], axis=1)
                w = w * (qj[p_old, :, cols] * mark)
                part = w[:, 0:128] + w[:, 128:256]
                row_part = part if row_part is None else row_part + part
                prod = lax.dot_general(xj[p_old, 0:feat, cols], w.astype(jnp.bfloat16), (((1,), (1,)), ((), ())),
                                       preferred_element_type=jnp.float32)
                pull = prod if pull is None else pull + prod
            acc[:, rows] += pull
            rs[rows, :] += row_part

    for t in range(n_tiles):
        for jt in range(CHUNK // TILE):
            cross(0, t, jt, s1)

    def pass_on(p):
        for k in range(len(FIRSTS), len(SENDS)):
            if POS[SENDS[k][0]] == p:
                for copy in copies(k):
                    copy.start()

    forward_at = sorted({POS[f[0]] for f in FORWARDS})

    def pair(i, carry):
        p1, p2 = 2 * i + 1, 2 * i + 2

        @pl.when(p1 >= PARTS)
        def _():
            arrived(p1)

        @pl.when(p2 >= PARTS)
        def _():
            arrived(p2)

        for f in sorted({(fp - 1) // 2 for fp in forward_at}):
            @pl.when(i == f)
            def _():
                for fp in forward_at:
                    if (fp - 1) // 2 == f:
                        pass_on(fp)

        phase(p1, s0, p1 - 1, s1)
        phase(p2, s1, p1, s0)
        return carry

    lax.fori_loop(0, (N_CHUNK - 2) // 2, pair, 0)
    arrived(N_CHUNK - 1)
    phase(N_CHUNK - 1, s0, N_CHUNK - 2, s1)
    phase(None, None, N_CHUNK - 1, s0)

    eslot[me] = 0.5 * jnp.sum(rs[...].reshape(n_rows // 8, 8, 128), axis=0)

    def out_copy(t):
        cols = slice(t * TILE, (t + 1) * TILE)
        return pltpu.make_async_copy(acc.at[:, cols], out_ref.at[:, cols], out_sem.at[t])

    def finish(t):
        for r0 in (t * TILE, t * TILE + 128):
            rows = slice(r0, r0 + 128)
            total = jnp.sum(rs[rows, :].T, axis=0, keepdims=True)
            acc[:, rows] = (total * x_ref[:, rows].astype(jnp.float32) - acc[:, rows]) * inv_lsq
        out_copy(t).start()

    def energy_copy(step):
        return pltpu.make_async_remote_copy(
            src_ref=eslot.at[me], dst_ref=eslot.at[me], send_sem=send_e.at[step - 1],
            recv_sem=recv_e.at[step - 1], device_id=(my_sys, lax.rem(me + step, 8)), device_id_type=MESH)

    finish(0)
    for step in range(1, 8):
        energy_copy(step).start()
    for t in range(1, n_tiles):
        finish(t)
    for k in range(len(SENDS)):
        for copy in copies(k):
            copy.wait_send()
    for step in range(1, 8):
        energy_copy(step).wait_send()
        src = lax.rem(me - step + 8, 8)
        pltpu.make_async_remote_copy(
            src_ref=eslot.at[src], dst_ref=eslot.at[src], send_sem=send_e.at[step - 1],
            recv_sem=recv_e.at[step - 1], device_id=(my_sys, me), device_id_type=MESH).wait_recv()
    total = eslot[0]
    for d in range(1, 8):
        total = total + eslot[d]
    en_ref[0] = jnp.sum(total)
    for t in range(n_tiles):
        out_copy(t).wait()


def solution(mesh):
    def device_fn(positions, charges, pair_band):
        n_rows, feat = positions.shape
        depth = feat + 8
        vmem = pl.BlockSpec(memory_space=pltpu.VMEM)
        f32, bf16 = jnp.float32, jnp.bfloat16
        dma = pltpu.SemaphoreType.DMA
        forces, energy = pl.pallas_call(
            functools.partial(kernel, 1.0 / feat),
            out_shape=[jax.ShapeDtypeStruct((feat, n_rows), f32), jax.ShapeDtypeStruct((1,), f32)],
            in_specs=[vmem, vmem, pl.BlockSpec(memory_space=pltpu.SMEM)],
            out_specs=[pl.BlockSpec(memory_space=pltpu.HBM), pl.BlockSpec(memory_space=pltpu.SMEM)],
            scratch_shapes=[
                pltpu.VMEM((n_rows, 384), bf16),
                pltpu.VMEM((N_CHUNK, depth, CHUNK), bf16),
                pltpu.VMEM((N_CHUNK, 1, CHUNK), f32),
                pltpu.VMEM((n_rows, 128), f32),
                pltpu.VMEM((CHUNK // TILE, n_rows, TILE), f32),
                pltpu.VMEM((CHUNK // TILE, n_rows, TILE), f32),
                pltpu.VMEM((feat, n_rows), f32),
                pltpu.VMEM((n_rows, 128), f32),
                pltpu.VMEM((2, TILE, TILE), f32),
                pltpu.VMEM((8, 8, 128), f32),
                pltpu.SMEM((N_CHUNK,), f32),
                pltpu.VMEM((8, n_rows), f32),
                dma((len(SENDS),)), dma((N_CHUNK,)), dma((len(SENDS),)), dma((N_CHUNK,)),
                dma((7,)), dma((7,)), dma((n_rows // TILE,)),
            ],
            compiler_params=pltpu.CompilerParams(
                collective_id=0, has_side_effects=True, vmem_limit_bytes=60 * 1024 * 1024),
            name='pair_forces',
        )(positions.T, charges.reshape(1, n_rows), pair_band)
        return forces.T, energy

    row_spec = P(('sys', 'seg'), None)
    vec_spec = P(('sys', 'seg'))
    return jax.shard_map(device_fn, mesh=mesh, in_specs=(row_spec, vec_spec, row_spec),
                         out_specs=(row_spec, P('sys')), check_vma=False)
```

```python
import functools

import jax
import jax.numpy as jnp
from jax import lax
from jax.experimental import pallas as pl
from jax.experimental.pallas import tpu as pltpu
from jax.sharding import PartitionSpec as P

MESH = pl.DeviceIdType.MESH
LOG2E = 1.4426950408889634
CHUNK = 512
TILE = 256
PARTS = 4
ORDER = [(0, c) for c in range(4)] + [(1, c) for c in range(4)] + [
    (2, 0), (4, 0), (3, 0), (2, 1), (4, 1), (3, 1), (2, 2), (4, 2), (3, 2), (2, 3), (4, 3), (3, 3),
    (6, 0), (5, 2), (5, 0), (6, 2), (6, 1), (5, 3), (5, 1), (6, 3)]
POS = {rc: i for i, rc in enumerate(ORDER)}
N_CHUNK = len(ORDER)
FORWARDS = (
    [((2, c), 'core', (3, c)) for c in range(4)]
    + [((4, c), 'x', (6, c)) for c in range(2)]
    + [((2, c), 'y', (5, c)) for c in range(2, 4)]
    + [((6, c), 'core', (5, c)) for c in range(2)]
    + [((5, c), 'core', (6, c)) for c in range(2, 4)])
FIRSTS = [((0, c), link, (role, c)) for c in range(4) for link, role in (('x', 2), ('yo', 4), ('core', 1))]
SENDS = FIRSTS + FORWARDS


def split3(v):
    hi = v.astype(jnp.bfloat16)
    rest = v - hi.astype(jnp.float32)
    mid = rest.astype(jnp.bfloat16)
    low = (rest - mid.astype(jnp.float32)).astype(jnp.bfloat16)
    return hi.astype(jnp.float32), mid.astype(jnp.float32), low.astype(jnp.float32)


def kernel(inv_lsq, x_ref, q_ref, band_ref, out_ref, en_ref,
           xi, xj, qj, qi, s0, s1, acc, rs, bound, eslot, mpos, aux,
           send_x, recv_x, send_q, recv_q, send_e, recv_e):
    feat, n_rows = x_ref.shape
    depth = xj.shape[1]
    n_tiles = n_rows // TILE
    scale = LOG2E * inv_lsq
    my_sys = lax.axis_index('sys')
    me = lax.axis_index('seg')
    core = lax.rem(me, 2)
    xc = lax.rem(me // 2, 2)
    yc = me // 4

    def dev(y, x, c):
        return (y * 2 + x) * 2 + c

    owner = {0: me, 1: dev(yc, xc, 1 - core), 2: dev(yc, 1 - xc, core), 3: dev(yc, 1 - xc, 1 - core),
             4: dev(1 - yc, xc, 1 - core), 5: dev(1 - yc, 1 - xc, core), 6: dev(1 - yc, 1 - xc, 1 - core)}
    target = {'core': owner[1], 'x': owner[2], 'yo': owner[4], 'y': dev(1 - yc, xc, core)}

    barrier = pltpu.get_barrier_semaphore()
    for step in range(1, 8):
        pl.semaphore_signal(barrier, inc=1, device_id=(my_sys, lax.rem(me + step, 8)), device_id_type=MESH)

    def copies(k):
        src, link, dst = SENDS[k]
        s, d = POS[src], POS[dst]
        to = (my_sys, target[link])
        return (
            pltpu.make_async_remote_copy(src_ref=qj.at[s], dst_ref=qj.at[d], send_sem=send_q.at[k],
                                         recv_sem=recv_q.at[d], device_id=to, device_id_type=MESH),
            pltpu.make_async_remote_copy(src_ref=xj.at[s], dst_ref=xj.at[d], send_sem=send_x.at[k],
                                         recv_sem=recv_x.at[d], device_id=to, device_id_type=MESH))

    def arrived(p):
        to = (my_sys, me)
        pltpu.make_async_remote_copy(src_ref=qj.at[p], dst_ref=qj.at[p], send_sem=send_q.at[0],
                                     recv_sem=recv_q.at[p], device_id=to, device_id_type=MESH).wait_recv()
        pltpu.make_async_remote_copy(src_ref=xj.at[p], dst_ref=xj.at[p], send_sem=send_x.at[0],
                                     recv_sem=recv_x.at[p], device_id=to, device_id_type=MESH).wait_recv()

    row8 = lax.broadcasted_iota(jnp.int32, (8, CHUNK), 0)
    extra_i = []
    for c in range(PARTS):
        cols = slice(c * CHUNK, (c + 1) * CHUNK)
        x_c = x_ref[:, cols]
        xj[c, 0:feat, :] = x_c
        x_f = x_c.astype(jnp.float32)
        pieces = split3(-0.5 * jnp.sum(x_f * x_f, axis=0, keepdims=True))
        v_j = jnp.where((row8 >= 3) & (row8 < 6), 1.0, 0.0)
        v_i = jnp.where(row8 < 3, 1.0, 0.0)
        for k in range(3):
            v_j = jnp.where(row8 == k, pieces[k], v_j)
            v_i = jnp.where(row8 == 3 + k, pieces[k], v_i)
        xj[c, feat:depth, :] = v_j.astype(jnp.bfloat16)
        aux[:, cols] = v_i
        qj[c] = q_ref[:, cols]

    pl.semaphore_wait(barrier, 7)
    for k in range(len(FIRSTS)):
        for copy in copies(k):
            copy.start()

    for g in range(n_rows // 128):
        rows = slice(g * 128, (g + 1) * 128)
        xi[rows, 0:128] = x_ref[0:128, rows].T
        xi[rows, 128:256] = x_ref[128:256, rows].T
        last = jnp.concatenate([x_ref[256:feat, rows].astype(jnp.float32), aux[:, rows],
                                jnp.zeros((384 - depth, 128), jnp.float32)], axis=0)
        xi[rows, 256:384] = last.T.astype(jnp.bfloat16)
        qi[rows, :] = jnp.broadcast_to(q_ref[:, rows], (128, 128)).T

    tr = lax.broadcasted_iota(jnp.int32, (TILE, TILE), 0)
    tc = lax.broadcasted_iota(jnp.int32, (TILE, TILE), 1)
    bound[0] = jnp.zeros((TILE, TILE), jnp.float32)
    bound[1] = jnp.where(tr == tc, -1e30, 0.0)
    acc[...] = jnp.zeros_like(acc)
    rs[...] = jnp.zeros_like(rs)
    for p, (role, _) in enumerate(ORDER):
        mpos[p] = band_ref[0, lax.rem(owner[role] - me + 11, 8)].astype(jnp.float32)

    def cross(p, t, jt, s_new):
        rows, cols = slice(t * TILE, (t + 1) * TILE), slice(jt * TILE, (jt + 1) * TILE)
        s_new[jt, rows, :] = jnp.dot(xi[rows, 0:depth], xj[p, :, cols], preferred_element_type=jnp.float32)

    def phase(p_new, s_new, p_old, s_old):
        mark = None if p_old is None else mpos[p_old]
        for t in range(n_tiles):
            rows = slice(t * TILE, (t + 1) * TILE)
            row_part, pull = None, None
            for jt in range(CHUNK // TILE):
                cols = slice(jt * TILE, (jt + 1) * TILE)
                if s_new is not None:
                    cross(p_new, t, jt, s_new)
                s = s_old[jt, rows, :]
                if t % 2 == jt:
                    top = bound[jnp.where(p_old == t // 2, 1, 0)]
                else:
                    top = 0.0
                e = jnp.exp2(jnp.minimum(s, top) * scale)
                q_rows = qi[rows, :]
                w = jnp.concatenate([e[:, 0:128] * q_rows, e[:, 128:256] * q_rows], axis=1)
                w = w * (qj[p_old, :, cols] * mark)
                part = w[:, 0:128] + w[:, 128:256]
                row_part = part if row_part is None else row_part + part
                prod = lax.dot_general(xj[p_old, 0:feat, cols], w.astype(jnp.bfloat16), (((1,), (1,)), ((), ())),
                                       preferred_element_type=jnp.float32)
                pull = prod if pull is None else pull + prod
            acc[:, rows] += pull
            rs[rows, :] += row_part

    for t in range(n_tiles):
        for jt in range(CHUNK // TILE):
            cross(0, t, jt, s1)

    def pass_on(p):
        for k in range(len(FIRSTS), len(SENDS)):
            if POS[SENDS[k][0]] == p:
                for copy in copies(k):
                    copy.start()

    forward_at = sorted({POS[f[0]] for f in FORWARDS})

    def pair(i, carry):
        p1, p2 = 2 * i + 1, 2 * i + 2

        @pl.when(p1 >= PARTS)
        def _():
            arrived(p1)

        @pl.when(p2 >= PARTS)
        def _():
            arrived(p2)

        for f in sorted({(fp - 1) // 2 for fp in forward_at}):
            @pl.when(i == f)
            def _():
                for fp in forward_at:
                    if (fp - 1) // 2 == f:
                        pass_on(fp)

        phase(p1, s0, p1 - 1, s1)
        phase(p2, s1, p1, s0)
        return carry

    lax.fori_loop(0, (N_CHUNK - 2) // 2, pair, 0)
    arrived(N_CHUNK - 1)
    phase(N_CHUNK - 1, s0, N_CHUNK - 2, s1)
    phase(None, None, N_CHUNK - 1, s0)

    eslot[me] = 0.5 * jnp.sum(rs[...].reshape(n_rows // 8, 8, 128), axis=0)

    def finish(t):
        for r0 in (t * TILE, t * TILE + 128):
            rows = slice(r0, r0 + 128)
            total = jnp.sum(rs[rows, :].T, axis=0, keepdims=True)
            out_ref[:, rows] = (total * x_ref[:, rows].astype(jnp.float32) - acc[:, rows]) * inv_lsq

    def energy_copy(step):
        return pltpu.make_async_remote_copy(
            src_ref=eslot.at[me], dst_ref=eslot.at[me], send_sem=send_e.at[step - 1],
            recv_sem=recv_e.at[step - 1], device_id=(my_sys, lax.rem(me + step, 8)), device_id_type=MESH)

    finish(0)
    for step in range(1, 8):
        energy_copy(step).start()
    for t in range(1, n_tiles):
        finish(t)
    for k in range(len(SENDS)):
        for copy in copies(k):
            copy.wait_send()
    for step in range(1, 8):
        energy_copy(step).wait_send()
        src = lax.rem(me - step + 8, 8)
        pltpu.make_async_remote_copy(
            src_ref=eslot.at[src], dst_ref=eslot.at[src], send_sem=send_e.at[step - 1],
            recv_sem=recv_e.at[step - 1], device_id=(my_sys, me), device_id_type=MESH).wait_recv()
    total = eslot[0]
    for d in range(1, 8):
        total = total + eslot[d]
    en_ref[0] = jnp.sum(total)


def solution(mesh):
    def device_fn(positions, charges, pair_band):
        n_rows, feat = positions.shape
        depth = feat + 8
        vmem = pl.BlockSpec(memory_space=pltpu.VMEM)
        f32, bf16 = jnp.float32, jnp.bfloat16
        dma = pltpu.SemaphoreType.DMA
        forces, energy = pl.pallas_call(
            functools.partial(kernel, 1.0 / feat),
            out_shape=[pltpu.VMEM((feat, n_rows), f32), jax.ShapeDtypeStruct((1,), f32)],
            in_specs=[vmem, vmem, pl.BlockSpec(memory_space=pltpu.SMEM)],
            out_specs=[vmem, pl.BlockSpec(memory_space=pltpu.SMEM)],
            scratch_shapes=[
                pltpu.VMEM((n_rows, 384), bf16),
                pltpu.VMEM((N_CHUNK, depth, CHUNK), bf16),
                pltpu.VMEM((N_CHUNK, 1, CHUNK), f32),
                pltpu.VMEM((n_rows, 128), f32),
                pltpu.VMEM((CHUNK // TILE, n_rows, TILE), f32),
                pltpu.VMEM((CHUNK // TILE, n_rows, TILE), f32),
                pltpu.VMEM((feat, n_rows), f32),
                pltpu.VMEM((n_rows, 128), f32),
                pltpu.VMEM((2, TILE, TILE), f32),
                pltpu.VMEM((8, 8, 128), f32),
                pltpu.SMEM((N_CHUNK,), f32),
                pltpu.VMEM((8, n_rows), f32),
                dma((len(SENDS),)), dma((N_CHUNK,)), dma((len(SENDS),)), dma((N_CHUNK,)),
                dma((7,)), dma((7,)),
            ],
            compiler_params=pltpu.CompilerParams(
                collective_id=0, has_side_effects=True, vmem_limit_bytes=40 * 1024 * 1024),
            name='pair_forces',
        )(positions.T, charges.reshape(1, n_rows), pair_band)
        return forces.T, energy

    row_spec = P(('sys', 'seg'), None)
    vec_spec = P(('sys', 'seg'))
    return jax.shard_map(device_fn, mesh=mesh, in_specs=(row_spec, vec_spec, row_spec),
                         out_specs=(row_spec, P('sys')), check_vma=False)
```

```python
import functools

import jax
import jax.numpy as jnp
from jax import lax
from jax.experimental import pallas as pl
from jax.experimental.pallas import tpu as pltpu
from jax.sharding import PartitionSpec as P

MESH = pl.DeviceIdType.MESH
LOG2E = 1.4426950408889634
CHUNK = 512
TILE = 256
PARTS = 4
ORDER = [(0, c) for c in range(4)] + [(1, c) for c in range(4)] + [
    (2, 0), (4, 0), (3, 0), (2, 1), (4, 1), (3, 1), (2, 2), (4, 2), (3, 2), (2, 3), (4, 3), (3, 3),
    (6, 0), (5, 2), (5, 0), (6, 2), (6, 1), (5, 3), (5, 1), (6, 3)]
POS = {rc: i for i, rc in enumerate(ORDER)}
N_CHUNK = len(ORDER)
FORWARDS = (
    [((2, c), 'core', (3, c)) for c in range(4)]
    + [((4, c), 'x', (6, c)) for c in range(2)]
    + [((2, c), 'y', (5, c)) for c in range(2, 4)]
    + [((6, c), 'core', (5, c)) for c in range(2)]
    + [((5, c), 'core', (6, c)) for c in range(2, 4)])
FIRSTS = [((0, c), link, (role, c)) for c in range(4) for link, role in (('x', 2), ('yo', 4), ('core', 1))]
SENDS = FIRSTS + FORWARDS


def split3(v):
    hi = v.astype(jnp.bfloat16)
    rest = v - hi.astype(jnp.float32)
    mid = rest.astype(jnp.bfloat16)
    low = (rest - mid.astype(jnp.float32)).astype(jnp.bfloat16)
    return hi.astype(jnp.float32), mid.astype(jnp.float32), low.astype(jnp.float32)


def kernel(inv_lsq, x_ref, q_ref, band_ref, out_ref, en_ref,
           xi, xj, qj, qi, s0, s1, acc, react, gift, rs, cs_own, cs_react, cs_gift, diag, eslot, band, mpos, aux,
           send_x, recv_x, send_q, recv_q, send_e, recv_e, send_g, recv_g, load_x, load_q, load_b):
    feat, n_rows = x_ref.shape
    depth = xj.shape[1]
    n_tiles = n_rows // TILE
    per_chunk = CHUNK // TILE
    scale = LOG2E * inv_lsq
    my_sys = lax.axis_index('sys')
    me = lax.axis_index('seg')
    core = lax.rem(me, 2)
    xc = lax.rem(me // 2, 2)
    yc = me // 4

    def dev(y, x, c):
        return (y * 2 + x) * 2 + c

    owner = {0: me, 1: dev(yc, xc, 1 - core), 2: dev(yc, 1 - xc, core), 3: dev(yc, 1 - xc, 1 - core),
             4: dev(1 - yc, xc, 1 - core), 5: dev(1 - yc, 1 - xc, core), 6: dev(1 - yc, 1 - xc, 1 - core)}
    target = {'core': owner[1], 'x': owner[2], 'yo': owner[4], 'y': dev(1 - yc, xc, core)}

    barrier = pltpu.get_barrier_semaphore()
    for step in range(1, 8):
        pl.semaphore_signal(barrier, inc=1, device_id=(my_sys, lax.rem(me + step, 8)), device_id_type=MESH)

    def loads(c):
        cols = slice(c * CHUNK, (c + 1) * CHUNK)
        return (pltpu.make_async_copy(x_ref.at[:, cols], xj.at[c, pl.ds(0, feat), :], load_x.at[c]),
                pltpu.make_async_copy(q_ref.at[:, cols], qj.at[c], load_q.at[c]))

    band_load = pltpu.make_async_copy(band_ref, band, load_b)
    for c in range(PARTS):
        for copy in loads(c):
            copy.start()
    band_load.start()

    def copies(k):
        src, link, dst = SENDS[k]
        s, d = POS[src], POS[dst]
        to = (my_sys, target[link])
        return (
            pltpu.make_async_remote_copy(src_ref=qj.at[s], dst_ref=qj.at[d], send_sem=send_q.at[k],
                                         recv_sem=recv_q.at[d], device_id=to, device_id_type=MESH),
            pltpu.make_async_remote_copy(src_ref=xj.at[s], dst_ref=xj.at[d], send_sem=send_x.at[k],
                                         recv_sem=recv_x.at[d], device_id=to, device_id_type=MESH))

    def arrived(p):
        to = (my_sys, me)
        pltpu.make_async_remote_copy(src_ref=qj.at[p], dst_ref=qj.at[p], send_sem=send_q.at[0],
                                     recv_sem=recv_q.at[p], device_id=to, device_id_type=MESH).wait_recv()
        pltpu.make_async_remote_copy(src_ref=xj.at[p], dst_ref=xj.at[p], send_sem=send_x.at[0],
                                     recv_sem=recv_x.at[p], device_id=to, device_id_type=MESH).wait_recv()

    row8 = lax.broadcasted_iota(jnp.int32, (8, CHUNK), 0)
    extra_i = []
    for c in range(PARTS):
        cols = slice(c * CHUNK, (c + 1) * CHUNK)
        for copy in loads(c):
            copy.wait()
        x_f = xj[c, 0:feat, :].astype(jnp.float32)
        pieces = split3(-0.5 * jnp.sum(x_f * x_f, axis=0, keepdims=True))
        v_j = jnp.where((row8 >= 3) & (row8 < 6), 1.0, 0.0)
        v_i = jnp.where(row8 < 3, 1.0, 0.0)
        for k in range(3):
            v_j = jnp.where(row8 == k, pieces[k], v_j)
            v_i = jnp.where(row8 == 3 + k, pieces[k], v_i)
        xj[c, feat:depth, :] = v_j.astype(jnp.bfloat16)
        aux[:, cols] = v_i

    pl.semaphore_wait(barrier, 7)
    for k in range(len(FIRSTS)):
        for copy in copies(k):
            copy.start()

    for g in range(n_rows // 128):
        rows = slice(g * 128, (g + 1) * 128)
        c, l0 = g * 128 // CHUNK, g * 128 % CHUNK
        cols = slice(l0, l0 + 128)
        xi[rows, 0:128] = xj[c, 0:128, cols].T
        xi[rows, 128:256] = xj[c, 128:256, cols].T
        last = jnp.concatenate([xj[c, 256:feat, cols].astype(jnp.float32), aux[:, rows],
                                jnp.zeros((384 - depth, 128), jnp.float32)], axis=0)
        xi[rows, 256:384] = last.T.astype(jnp.bfloat16)
        qi[rows, :] = jnp.broadcast_to(qj[c, :, cols], (128, 128)).T

    tr = lax.broadcasted_iota(jnp.int32, (TILE, TILE), 0)
    tc = lax.broadcasted_iota(jnp.int32, (TILE, TILE), 1)
    diag[...] = jnp.where(tr == tc, -1e30, 0.0)
    for ref in (acc, react, rs, cs_own, cs_react):
        ref[...] = jnp.zeros_like(ref)
    band_load.wait()
    for p, (role, _) in enumerate(ORDER):
        mpos[p] = band[0, lax.rem(owner[role] - me + 11, 8)].astype(jnp.float32)

    half = n_tiles // 2
    own_steps = []
    for r in (1, 2, 3):
        a2 = 4 // (r + 1)
        own_steps.append([([2 * a, 2 * a + 1], b, b * CHUNK) for a, b in ((0, r), (a2, 6 - r - a2))])
    own_diag = [([2 * c, 2 * c + 1], c, None) for c in range(PARTS)]
    peer_steps = []
    for k in range(4):
        part = lax.rem(k // 2 + core, 2) * 2 + k % 2
        tiles = list(range(k // 2 * half, (k // 2 + 1) * half))
        peer_steps.append([(tiles, PARTS + part, pl.multiple_of(part * CHUNK, CHUNK))])

    def whole(p):
        return [(list(range(n_tiles)), p, None)]

    def crosses(step, s_new):
        def one(n, t, p, jt):
            rows, cols = slice(t * TILE, (t + 1) * TILE), slice(jt * TILE, (jt + 1) * TILE)
            s_new[n] = jnp.dot(xi[rows, 0:depth], xj[p, :, cols], preferred_element_type=jnp.float32)
        todo = [(t, p, jt) for tiles, p, _ in step for t in tiles for jt in range(per_chunk)]
        return [functools.partial(one, n, *args) for n, args in enumerate(todo)]

    def consume(step, s_old, masked=False, back=None, cs=None):
        n = 0
        for tiles, p, first in step:
            mark = mpos[p]
            pulls, sums = [None] * per_chunk, [None] * per_chunk
            for ti, t in enumerate(tiles):
                rows = slice(t * TILE, (t + 1) * TILE)
                t_lane = t * TILE % CHUNK
                row_part, pull = None, None
                for jt in range(per_chunk):
                    yield
                    cols = slice(jt * TILE, (jt + 1) * TILE)
                    top = diag[...] if masked and ti == jt else 0.0
                    e = jnp.exp2(jnp.minimum(s_old[n], top) * scale)
                    q_rows = qi[rows, :]
                    w = jnp.concatenate([e[:, 0:128] * q_rows, e[:, 128:256] * q_rows], axis=1)
                    w = w * (qj[p, :, cols] * mark)
                    part = w[:, 0:128] + w[:, 128:256]
                    row_part = part if row_part is None else row_part + part
                    w_low = w.astype(jnp.bfloat16)
                    prod = lax.dot_general(xj[p, 0:feat, cols], w_low, (((1,), (1,)), ((), ())),
                                           preferred_element_type=jnp.float32)
                    pull = prod if pull is None else pull + prod
                    if back is not None:
                        prod = jnp.dot(xj[t * TILE // CHUNK, 0:feat, t_lane:t_lane + TILE], w_low,
                                       preferred_element_type=jnp.float32)
                        pulls[jt] = prod if pulls[jt] is None else pulls[jt] + prod
                        part = jnp.sum(w.reshape(TILE // 8, 8, TILE), axis=0)
                        sums[jt] = part if sums[jt] is None else sums[jt] + part
                    n += 1
                acc[:, rows] += pull
                rs[rows, :] += row_part
            if back is not None:
                for jt in range(per_chunk):
                    cols = pl.ds(first + jt * TILE, TILE)
                    back[:, cols] += pulls[jt]
                    cs[:, cols] += sums[jt]

    def phase(new, eaten, n_eaten):
        given = 0
        for k, _ in enumerate(eaten):
            upto = -(-len(new) * (k + 1) // n_eaten)
            for f in new[given:upto]:
                f()
            given = max(given, upto)

    for f in crosses(own_steps[0], s1):
        f()
    own = dict(back=acc, cs=cs_own)
    peer = dict(back=react, cs=cs_react)
    phase(crosses(own_steps[1], s0), consume(own_steps[0], s1, **own), 8)
    phase(crosses(own_steps[2], s1), consume(own_steps[1], s0, **own), 8)
    phase(crosses(own_diag, s0), consume(own_steps[2], s1, **own), 8)
    for c in range(PARTS):
        arrived(PARTS + c)
    phase(crosses(peer_steps[0], s1), consume(own_diag, s0, masked=True), 16)
    phase(crosses(peer_steps[1], s0), consume(peer_steps[0], s1, **peer), 8)
    arrived(2 * PARTS)

    def pass_on(p):
        for k in range(len(FIRSTS), len(SENDS)):
            if POS[SENDS[k][0]] == p:
                for copy in copies(k):
                    copy.start()

    pass_on(2 * PARTS)
    phase(crosses(peer_steps[2], s1), consume(peer_steps[1], s0, **peer), 8)
    phase(crosses(peer_steps[3], s0), consume(peer_steps[2], s1, **peer), 8)
    phase(crosses(whole(2 * PARTS), s1), consume(peer_steps[3], s0, **peer), 8)

    def gifts():
        to = (my_sys, owner[1])
        return (
            pltpu.make_async_remote_copy(src_ref=react, dst_ref=gift, send_sem=send_g.at[0],
                                         recv_sem=recv_g.at[0], device_id=to, device_id_type=MESH),
            pltpu.make_async_remote_copy(src_ref=cs_react, dst_ref=cs_gift, send_sem=send_g.at[1],
                                         recv_sem=recv_g.at[1], device_id=to, device_id_type=MESH))

    forward_at = sorted({POS[f[0]] for f in FORWARDS})

    def pair(i, carry):
        p1, p2 = 2 * i + 2 * PARTS + 1, 2 * i + 2 * PARTS + 2
        arrived(p1)
        arrived(p2)
        for f in range((N_CHUNK - 2 * PARTS - 2) // 2):
            due = [fp for fp in forward_at if fp - 2 * PARTS in (2 * f + 1, 2 * f + 2)]
            if due or f == 1:
                @pl.when(i == f)
                def _():
                    for fp in due:
                        pass_on(fp)
                    if f == 1:
                        for copy in gifts():
                            copy.start()

        phase(crosses(whole(p1), s0), consume(whole(p1 - 1), s1), 16)
        phase(crosses(whole(p2), s1), consume(whole(p1), s0), 16)
        return carry

    lax.fori_loop(0, (N_CHUNK - 2 * PARTS - 2) // 2, pair, 0)
    arrived(N_CHUNK - 1)
    for copy in gifts():
        copy.wait_recv()
    phase(crosses(whole(N_CHUNK - 1), s0), consume(whole(N_CHUNK - 2), s1), 16)
    phase([], consume(whole(N_CHUNK - 1), s0), 16)

    own_part = jnp.sum(rs[...].reshape(n_rows // 8, 8, 128), axis=0)
    for g in range(n_rows // 128):
        own_part = own_part + cs_own[:, g * 128:(g + 1) * 128] + cs_react[:, g * 128:(g + 1) * 128]
    eslot[me] = 0.5 * own_part

    def finish(t):
        for r0 in (t * TILE, t * TILE + 128):
            rows = slice(r0, r0 + 128)
            c, l0 = r0 // CHUNK, r0 % CHUNK
            total = jnp.sum(rs[rows, :].T, axis=0, keepdims=True)
            total = total + jnp.sum(cs_own[:, rows] + cs_gift[:, rows], axis=0, keepdims=True)
            x_part = xj[c, 0:feat, l0:l0 + 128].astype(jnp.float32)
            out_ref[:, rows] = (total * x_part - (acc[:, rows] + gift[:, rows])) * inv_lsq

    def energy_copy(step):
        return pltpu.make_async_remote_copy(
            src_ref=eslot.at[me], dst_ref=eslot.at[me], send_sem=send_e.at[step - 1],
            recv_sem=recv_e.at[step - 1], device_id=(my_sys, lax.rem(me + step, 8)), device_id_type=MESH)

    finish(0)
    for step in range(1, 8):
        energy_copy(step).start()
    for t in range(1, n_tiles):
        finish(t)
    for k in range(len(SENDS)):
        for copy in copies(k):
            copy.wait_send()
    for copy in gifts():
        copy.wait_send()
    for step in range(1, 8):
        energy_copy(step).wait_send()
        src = lax.rem(me - step + 8, 8)
        pltpu.make_async_remote_copy(
            src_ref=eslot.at[src], dst_ref=eslot.at[src], send_sem=send_e.at[step - 1],
            recv_sem=recv_e.at[step - 1], device_id=(my_sys, me), device_id_type=MESH).wait_recv()
    total = eslot[0]
    for d in range(1, 8):
        total = total + eslot[d]
    en_ref[0] = jnp.sum(total)


def solution(mesh):
    def device_fn(positions, charges, pair_band):
        n_rows, feat = positions.shape
        depth = feat + 8
        vmem = pl.BlockSpec(memory_space=pltpu.VMEM)
        hbm = pl.BlockSpec(memory_space=pltpu.HBM)
        f32, bf16 = jnp.float32, jnp.bfloat16
        dma = pltpu.SemaphoreType.DMA
        forces, energy = pl.pallas_call(
            functools.partial(kernel, 1.0 / feat),
            out_shape=[pltpu.VMEM((feat, n_rows), f32), jax.ShapeDtypeStruct((1,), f32)],
            in_specs=[hbm, hbm, hbm],
            out_specs=[vmem, pl.BlockSpec(memory_space=pltpu.SMEM)],
            scratch_shapes=[
                pltpu.VMEM((n_rows, 384), bf16),
                pltpu.VMEM((N_CHUNK, depth, CHUNK), bf16),
                pltpu.VMEM((N_CHUNK, 1, CHUNK), f32),
                pltpu.VMEM((n_rows, 128), f32),
                pltpu.VMEM((n_rows // 128, TILE, TILE), f32),
                pltpu.VMEM((n_rows // 128, TILE, TILE), f32),
                pltpu.VMEM((feat, n_rows), f32),
                pltpu.VMEM((feat, n_rows), f32),
                pltpu.VMEM((feat, n_rows), f32),
                pltpu.VMEM((n_rows, 128), f32),
                pltpu.VMEM((8, n_rows), f32),
                pltpu.VMEM((8, n_rows), f32),
                pltpu.VMEM((8, n_rows), f32),
                pltpu.VMEM((TILE, TILE), f32),
                pltpu.VMEM((8, 8, 128), f32),
                pltpu.SMEM(pair_band.shape, jnp.int32),
                pltpu.SMEM((N_CHUNK,), f32),
                pltpu.VMEM((8, n_rows), f32),
                dma((len(SENDS),)), dma((N_CHUNK,)), dma((len(SENDS),)), dma((N_CHUNK,)),
                dma((7,)), dma((7,)), dma((2,)), dma((2,)), dma((PARTS,)), dma((PARTS,)), dma,
            ],
            compiler_params=pltpu.CompilerParams(
                collective_id=0, has_side_effects=True, vmem_limit_bytes=64421888),
            name='pair_forces',
        )(positions.T, charges.reshape(1, n_rows), pair_band)
        return forces.T, energy

    row_spec = P(('sys', 'seg'), None)
    vec_spec = P(('sys', 'seg'))
    return jax.shard_map(device_fn, mesh=mesh, in_specs=(row_spec, vec_spec, row_spec),
                         out_specs=(row_spec, P('sys')), check_vma=False)
```

```python
import functools

import jax
import jax.numpy as jnp
from jax import lax
from jax.experimental import pallas as pl
from jax.experimental.pallas import tpu as pltpu
from jax.sharding import PartitionSpec as P

MESH = pl.DeviceIdType.MESH
LOG2E = 1.4426950408889634
CHUNK = 512
TILE = 256
PARTS = 4
ORDER = [(0, c) for c in range(4)] + [(1, c) for c in range(4)] + [
    (2, 2), (4, 0), (3, 2), (2, 3), (4, 1), (3, 3), (6, 0), (5, 2), (5, 0), (6, 2),
    (6, 1), (5, 3), (5, 1), (6, 3), (2, 0), (4, 2), (3, 0), (2, 1), (4, 3), (3, 1)]
POS = {rc: i for i, rc in enumerate(ORDER)}
N_CHUNK = len(ORDER)
FORWARDS = (
    [((2, c), 'core', (3, c)) for c in range(4)]
    + [((4, c), 'x', (6, c)) for c in range(2)]
    + [((2, c), 'y', (5, c)) for c in range(2, 4)]
    + [((6, c), 'core', (5, c)) for c in range(2)]
    + [((5, c), 'core', (6, c)) for c in range(2, 4)])
FIRSTS = [((0, c), link, (role, c)) for link, role, c in (
    ('x', 2, 2), ('yo', 4, 0), ('core', 1, 0), ('x', 2, 3), ('yo', 4, 1), ('core', 1, 1), ('core', 1, 2), ('core', 1, 3))]
LATER = [((0, c), link, (role, c)) for link, role, c in (('x', 2, 0), ('yo', 4, 2), ('x', 2, 1), ('yo', 4, 3))]
SENDS = FIRSTS + FORWARDS + LATER


def split3(v):
    hi = v.astype(jnp.bfloat16)
    rest = v - hi.astype(jnp.float32)
    mid = rest.astype(jnp.bfloat16)
    low = (rest - mid.astype(jnp.float32)).astype(jnp.bfloat16)
    return hi.astype(jnp.float32), mid.astype(jnp.float32), low.astype(jnp.float32)


def kernel(inv_lsq, x_ref, q_ref, band_ref, out_ref, en_ref,
           xi, xj, qj, qi, s0, s1, acc, react, gift, rs, cs_own, cs_react, cs_gift, diag, eslot, eacc, band, mpos, epos, aux,
           send_x, recv_x, send_q, recv_q, send_e, recv_e, send_g, recv_g, load_x, load_q, load_b):
    feat, n_rows = x_ref.shape
    depth = xj.shape[1]
    n_tiles = n_rows // TILE
    per_chunk = CHUNK // TILE
    scale = LOG2E * inv_lsq
    my_sys = lax.axis_index('sys')
    me = lax.axis_index('seg')
    core = lax.rem(me, 2)
    xc = lax.rem(me // 2, 2)
    yc = me // 4

    def dev(y, x, c):
        return (y * 2 + x) * 2 + c

    owner = {0: me, 1: dev(yc, xc, 1 - core), 2: dev(yc, 1 - xc, core), 3: dev(yc, 1 - xc, 1 - core),
             4: dev(1 - yc, xc, 1 - core), 5: dev(1 - yc, 1 - xc, core), 6: dev(1 - yc, 1 - xc, 1 - core)}
    target = {'core': owner[1], 'x': owner[2], 'yo': owner[4], 'y': dev(1 - yc, xc, core)}

    barrier = pltpu.get_barrier_semaphore()
    for step in range(1, 8):
        pl.semaphore_signal(barrier, inc=1, device_id=(my_sys, lax.rem(me + step, 8)), device_id_type=MESH)

    def loads(c):
        cols = slice(c * CHUNK, (c + 1) * CHUNK)
        return (pltpu.make_async_copy(x_ref.at[:, cols], xj.at[c, pl.ds(0, feat), :], load_x.at[c]),
                pltpu.make_async_copy(q_ref.at[:, cols], qj.at[c], load_q.at[c]))

    band_load = pltpu.make_async_copy(band_ref, band, load_b)
    for c in range(PARTS):
        for copy in loads(c):
            copy.start()
    band_load.start()

    def copies(k):
        src, link, dst = SENDS[k]
        s, d = POS[src], POS[dst]
        to = (my_sys, target[link])
        return (
            pltpu.make_async_remote_copy(src_ref=qj.at[s], dst_ref=qj.at[d], send_sem=send_q.at[k],
                                         recv_sem=recv_q.at[d], device_id=to, device_id_type=MESH),
            pltpu.make_async_remote_copy(src_ref=xj.at[s], dst_ref=xj.at[d], send_sem=send_x.at[k],
                                         recv_sem=recv_x.at[d], device_id=to, device_id_type=MESH))

    def arrived(p):
        to = (my_sys, me)
        pltpu.make_async_remote_copy(src_ref=qj.at[p], dst_ref=qj.at[p], send_sem=send_q.at[0],
                                     recv_sem=recv_q.at[p], device_id=to, device_id_type=MESH).wait_recv()
        pltpu.make_async_remote_copy(src_ref=xj.at[p], dst_ref=xj.at[p], send_sem=send_x.at[0],
                                     recv_sem=recv_x.at[p], device_id=to, device_id_type=MESH).wait_recv()

    row8 = lax.broadcasted_iota(jnp.int32, (8, CHUNK), 0)
    extra_i = []
    for c in range(PARTS):
        cols = slice(c * CHUNK, (c + 1) * CHUNK)
        for copy in loads(c):
            copy.wait()
        x_f = xj[c, 0:feat, :].astype(jnp.float32)
        pieces = split3(-0.5 * jnp.sum(x_f * x_f, axis=0, keepdims=True))
        v_j = jnp.where((row8 >= 3) & (row8 < 6), 1.0, 0.0)
        v_i = jnp.where(row8 < 3, 1.0, 0.0)
        for k in range(3):
            v_j = jnp.where(row8 == k, pieces[k], v_j)
            v_i = jnp.where(row8 == 3 + k, pieces[k], v_i)
        xj[c, feat:depth, :] = v_j.astype(jnp.bfloat16)
        aux[:, cols] = v_i

    pl.semaphore_wait(barrier, 7)
    for k in range(len(FIRSTS)):
        for copy in copies(k):
            copy.start()

    for g in range(n_rows // 128):
        rows = slice(g * 128, (g + 1) * 128)
        c, l0 = g * 128 // CHUNK, g * 128 % CHUNK
        cols = slice(l0, l0 + 128)
        xi[rows, 0:128] = xj[c, 0:128, cols].T
        xi[rows, 128:256] = xj[c, 128:256, cols].T
        last = jnp.concatenate([xj[c, 256:feat, cols].astype(jnp.float32), aux[:, rows],
                                jnp.zeros((384 - depth, 128), jnp.float32)], axis=0)
        xi[rows, 256:384] = last.T.astype(jnp.bfloat16)
        qi[rows, :] = jnp.broadcast_to(qj[c, :, cols], (128, 128)).T

    tr = lax.broadcasted_iota(jnp.int32, (TILE, TILE), 0)
    tc = lax.broadcasted_iota(jnp.int32, (TILE, TILE), 1)
    diag[...] = jnp.where(tr == tc, -1e30, 0.0)
    for ref in (acc, react, rs, cs_own, cs_react, eacc):
        ref[...] = jnp.zeros_like(ref)
    band_load.wait()
    for p, (role, _) in enumerate(ORDER):
        mpos[p] = band[0, lax.rem(owner[role] - me + 11, 8)].astype(jnp.float32)

    on_core = core.astype(jnp.float32)
    share = {3: 1.0 - on_core, 4: on_core}
    for p, (role, _) in enumerate(ORDER):
        epos[p] = share.get(role, 0.5 * jnp.ones_like(on_core))

    half = n_tiles // 2
    own_steps = []
    for r in (1, 2, 3):
        a2 = 4 // (r + 1)
        own_steps.append([([2 * a, 2 * a + 1], b, b * CHUNK) for a, b in ((0, r), (a2, 6 - r - a2))])
    own_diag = [([2 * c, 2 * c + 1], c, None) for c in range(PARTS)]
    peer_steps = []
    for k in range(4):
        part = lax.rem(k // 2 + core, 2) * 2 + k % 2
        tiles = list(range(k // 2 * half, (k // 2 + 1) * half))
        peer_steps.append([(tiles, PARTS + part, pl.multiple_of(part * CHUNK, CHUNK))])

    def whole(p):
        return [(list(range(n_tiles)), p, None)]

    def crosses(step, s_new):
        def one(n, t, p, jt):
            rows, cols = slice(t * TILE, (t + 1) * TILE), slice(jt * TILE, (jt + 1) * TILE)
            s_new[n] = jnp.dot(xi[rows, 0:depth], xj[p, :, cols], preferred_element_type=jnp.float32)
        todo = [(t, p, jt) for tiles, p, _ in step for t in tiles for jt in range(per_chunk)]
        return [functools.partial(one, n, *args) for n, args in enumerate(todo)]

    def consume(step, s_old, masked=False, back=None, cs=None, weight=None):
        n = 0
        for tiles, p, first in step:
            mark = mpos[p]
            pulls, sums = [None] * per_chunk, [None] * per_chunk
            e_part = jnp.zeros((8, 128), jnp.float32)
            for ti, t in enumerate(tiles):
                rows = slice(t * TILE, (t + 1) * TILE)
                t_lane = t * TILE % CHUNK
                row_part, pull = None, None
                for jt in range(per_chunk):
                    yield
                    cols = slice(jt * TILE, (jt + 1) * TILE)
                    top = diag[...] if masked and ti == jt else 0.0
                    e = jnp.exp2(jnp.minimum(s_old[n], top) * scale)
                    q_rows = qi[rows, :]
                    w = jnp.concatenate([e[:, 0:128] * q_rows, e[:, 128:256] * q_rows], axis=1)
                    w = w * (qj[p, :, cols] * mark)
                    part = w[:, 0:128] + w[:, 128:256]
                    row_part = part if row_part is None else row_part + part
                    w_low = w.astype(jnp.bfloat16)
                    prod = lax.dot_general(xj[p, 0:feat, cols], w_low, (((1,), (1,)), ((), ())),
                                           preferred_element_type=jnp.float32)
                    pull = prod if pull is None else pull + prod
                    if back is not None:
                        prod = jnp.dot(xj[t * TILE // CHUNK, 0:feat, t_lane:t_lane + TILE], w_low,
                                       preferred_element_type=jnp.float32)
                        pulls[jt] = prod if pulls[jt] is None else pulls[jt] + prod
                        part = jnp.sum(w.reshape(TILE // 8, 8, TILE), axis=0)
                        sums[jt] = part if sums[jt] is None else sums[jt] + part
                    n += 1
                acc[:, rows] += pull
                rs[rows, :] += row_part
                e_part = e_part + jnp.sum(row_part.reshape(TILE // 8, 8, 128), axis=0)
            eacc[...] += e_part * (epos[p] if weight is None else weight)
            if back is not None:
                for jt in range(per_chunk):
                    cols = pl.ds(first + jt * TILE, TILE)
                    back[:, cols] += pulls[jt]
                    cs[:, cols] += sums[jt]

    def phase(new, eaten, n_eaten):
        given = 0
        for k, _ in enumerate(eaten):
            upto = -(-len(new) * (k + 1) // n_eaten)
            for f in new[given:upto]:
                f()
            given = max(given, upto)

    for f in crosses(own_steps[0], s1):
        f()
    own = dict(back=acc, cs=cs_own, weight=1.0)
    peer = dict(back=react, cs=cs_react, weight=1.0)
    phase(crosses(own_steps[1], s0), consume(own_steps[0], s1, **own), 8)
    phase(crosses(own_steps[2], s1), consume(own_steps[1], s0, **own), 8)
    phase(crosses(own_diag, s0), consume(own_steps[2], s1, **own), 8)
    for c in range(PARTS):
        arrived(PARTS + c)
    phase(crosses(peer_steps[0], s1), consume(own_diag, s0, masked=True, weight=0.5), 16)
    phase(crosses(peer_steps[1], s0), consume(peer_steps[0], s1, **peer), 8)
    phase(crosses(peer_steps[2], s1), consume(peer_steps[1], s0, **peer), 8)

    def pass_on(p):
        for k in range(len(FIRSTS), len(FIRSTS) + len(FORWARDS)):
            if POS[SENDS[k][0]] == p:
                for copy in copies(k):
                    copy.start()

    for p in (2 * PARTS, 2 * PARTS + 1):
        arrived(p)
        pass_on(p)
    phase(crosses(peer_steps[3], s0), consume(peer_steps[2], s1, **peer), 8)
    phase(crosses(whole(2 * PARTS), s1), consume(peer_steps[3], s0, **peer), 8)

    def gifts():
        to = (my_sys, owner[1])
        return (
            pltpu.make_async_remote_copy(src_ref=react, dst_ref=gift, send_sem=send_g.at[0],
                                         recv_sem=recv_g.at[0], device_id=to, device_id_type=MESH),
            pltpu.make_async_remote_copy(src_ref=cs_react, dst_ref=cs_gift, send_sem=send_g.at[1],
                                         recv_sem=recv_g.at[1], device_id=to, device_id_type=MESH))

    forward_at = sorted({POS[f[0]] for f in FORWARDS})

    n_pairs = (N_CHUNK - 2 * PARTS - 4) // 2

    def pair(i, carry):
        p1, p2 = 2 * i + 2 * PARTS + 1, 2 * i + 2 * PARTS + 2

        @pl.when(i > 0)
        def _():
            arrived(p1)

        arrived(p2)
        for f in range(n_pairs):
            due = [fp for fp in forward_at if fp - 2 * PARTS in (2 * f + 1, 2 * f + 2) and fp > 2 * PARTS + 1]
            if due or f == 1:
                @pl.when(i == f)
                def _():
                    for fp in due:
                        pass_on(fp)
                    if f == 1:
                        for k in range(len(FIRSTS) + len(FORWARDS), len(SENDS)):
                            for copy in copies(k):
                                copy.start()
                        for copy in gifts():
                            copy.start()

        phase(crosses(whole(p1), s0), consume(whole(p1 - 1), s1), 16)
        phase(crosses(whole(p2), s1), consume(whole(p1), s0), 16)
        return carry

    lax.fori_loop(0, n_pairs, pair, 0)
    p_late, p_end = N_CHUNK - 1 - core, N_CHUNK - 2 + core
    arrived(N_CHUNK - 3)
    pass_on(N_CHUNK - 3)
    phase(crosses(whole(N_CHUNK - 3), s0), consume(whole(N_CHUNK - 4), s1), 16)
    arrived(N_CHUNK - 2)
    arrived(N_CHUNK - 1)
    for copy in gifts():
        copy.wait_recv()
    phase(crosses(whole(p_late), s1), consume(whole(N_CHUNK - 3), s0), 16)
    phase(crosses(whole(p_end), s0), consume(whole(p_late), s1), 16)
    eslot[me] = eacc[...]

    def finish(t):
        for r0 in (t * TILE, t * TILE + 128):
            rows = slice(r0, r0 + 128)
            c, l0 = r0 // CHUNK, r0 % CHUNK
            total = jnp.sum(rs[rows, :].T, axis=0, keepdims=True)
            total = total + jnp.sum(cs_own[:, rows] + cs_gift[:, rows], axis=0, keepdims=True)
            x_part = xj[c, 0:feat, l0:l0 + 128].astype(jnp.float32)
            out_ref[:, rows] = (total * x_part - (acc[:, rows] + gift[:, rows])) * inv_lsq

    def energy_copy(step):
        return pltpu.make_async_remote_copy(
            src_ref=eslot.at[me], dst_ref=eslot.at[me], send_sem=send_e.at[step - 1],
            recv_sem=recv_e.at[step - 1], device_id=(my_sys, lax.rem(me + step, 8)), device_id_type=MESH)

    for n, _ in enumerate(consume(whole(p_end), s0)):
        if n == 6:
            for step in range(1, 8):
                energy_copy(step).start()
    for t in range(n_tiles):
        finish(t)
    for k in range(len(SENDS)):
        for copy in copies(k):
            copy.wait_send()
    for copy in gifts():
        copy.wait_send()
    for step in range(1, 8):
        energy_copy(step).wait_send()
        src = lax.rem(me - step + 8, 8)
        pltpu.make_async_remote_copy(
            src_ref=eslot.at[src], dst_ref=eslot.at[src], send_sem=send_e.at[step - 1],
            recv_sem=recv_e.at[step - 1], device_id=(my_sys, me), device_id_type=MESH).wait_recv()
    total = eslot[0]
    for d in range(1, 8):
        total = total + eslot[d]
    en_ref[0] = jnp.sum(total)


def solution(mesh):
    def device_fn(positions, charges, pair_band):
        n_rows, feat = positions.shape
        depth = feat + 8
        vmem = pl.BlockSpec(memory_space=pltpu.VMEM)
        hbm = pl.BlockSpec(memory_space=pltpu.HBM)
        f32, bf16 = jnp.float32, jnp.bfloat16
        dma = pltpu.SemaphoreType.DMA
        forces, energy = pl.pallas_call(
            functools.partial(kernel, 1.0 / feat),
            out_shape=[pltpu.VMEM((feat, n_rows), f32), jax.ShapeDtypeStruct((1,), f32)],
            in_specs=[hbm, hbm, hbm],
            out_specs=[vmem, pl.BlockSpec(memory_space=pltpu.SMEM)],
            scratch_shapes=[
                pltpu.VMEM((n_rows, 384), bf16),
                pltpu.VMEM((N_CHUNK, depth, CHUNK), bf16),
                pltpu.VMEM((N_CHUNK, 1, CHUNK), f32),
                pltpu.VMEM((n_rows, 128), f32),
                pltpu.VMEM((n_rows // 128, TILE, TILE), f32),
                pltpu.VMEM((n_rows // 128, TILE, TILE), f32),
                pltpu.VMEM((feat, n_rows), f32),
                pltpu.VMEM((feat, n_rows), f32),
                pltpu.VMEM((feat, n_rows), f32),
                pltpu.VMEM((n_rows, 128), f32),
                pltpu.VMEM((8, n_rows), f32),
                pltpu.VMEM((8, n_rows), f32),
                pltpu.VMEM((8, n_rows), f32),
                pltpu.VMEM((TILE, TILE), f32),
                pltpu.VMEM((8, 8, 128), f32),
                pltpu.VMEM((8, 128), f32),
                pltpu.SMEM(pair_band.shape, jnp.int32),
                pltpu.SMEM((N_CHUNK,), f32),
                pltpu.SMEM((N_CHUNK,), f32),
                pltpu.VMEM((8, n_rows), f32),
                dma((len(SENDS),)), dma((N_CHUNK,)), dma((len(SENDS),)), dma((N_CHUNK,)),
                dma((7,)), dma((7,)), dma((2,)), dma((2,)), dma((PARTS,)), dma((PARTS,)), dma,
            ],
            compiler_params=pltpu.CompilerParams(
                collective_id=0, has_side_effects=True, vmem_limit_bytes=64421888),
            name='pair_forces',
        )(positions.T, charges.reshape(1, n_rows), pair_band)
        return forces.T, energy

    row_spec = P(('sys', 'seg'), None)
    vec_spec = P(('sys', 'seg'))
    return jax.shard_map(device_fn, mesh=mesh, in_specs=(row_spec, vec_spec, row_spec),
                         out_specs=(row_spec, P('sys')), check_vma=False)
```

```python
import functools

import jax
import jax.numpy as jnp
from jax import lax
from jax.experimental import pallas as pl
from jax.experimental.pallas import tpu as pltpu
from jax.sharding import PartitionSpec as P

MESH = pl.DeviceIdType.MESH
LOG2E = 1.4426950408889634
CHUNK = 512
TILE = 256
PARTS = 4
ORDER = [(0, c) for c in range(4)] + [(1, c) for c in range(4)] + [
    (2, 2), (4, 0), (3, 2), (2, 3), (4, 1), (3, 3), (6, 0), (5, 2), (5, 0), (6, 2),
    (6, 1), (5, 3), (5, 1), (6, 3), (2, 0), (4, 2), (3, 0), (2, 1), (4, 3), (3, 1)]
POS = {rc: i for i, rc in enumerate(ORDER)}
N_CHUNK = len(ORDER)
FORWARDS = (
    [((2, c), 'core', (3, c)) for c in range(4)]
    + [((4, c), 'x', (6, c)) for c in range(2)]
    + [((2, c), 'y', (5, c)) for c in range(2, 4)]
    + [((6, c), 'core', (5, c)) for c in range(2)]
    + [((5, c), 'core', (6, c)) for c in range(2, 4)])
FIRSTS = [((0, c), link, (role, c)) for link, role, c in (
    ('x', 2, 2), ('yo', 4, 0), ('core', 1, 0), ('x', 2, 3), ('yo', 4, 1), ('core', 1, 1), ('core', 1, 2), ('core', 1, 3))]
LATER = [((0, c), link, (role, c)) for link, role, c in (('x', 2, 0), ('yo', 4, 2), ('x', 2, 1), ('yo', 4, 3))]
SENDS = FIRSTS + FORWARDS + LATER


def split3(v):
    hi = v.astype(jnp.bfloat16)
    rest = v - hi.astype(jnp.float32)
    mid = rest.astype(jnp.bfloat16)
    low = (rest - mid.astype(jnp.float32)).astype(jnp.bfloat16)
    return hi.astype(jnp.float32), mid.astype(jnp.float32), low.astype(jnp.float32)


def kernel(inv_lsq, x_ref, q_ref, band_ref, out_ref, en_ref,
           xi, xj, qj, qi, s0, s1, acc, react, gift, rs, cs_own, cs_react, cs_gift, diag, eslot, eacc, band, mpos, epos, aux,
           send_x, recv_x, send_q, recv_q, send_e, recv_e, send_g, recv_g, load_x, load_q, load_b):
    feat, n_rows = x_ref.shape
    depth = xj.shape[1]
    n_tiles = n_rows // TILE
    per_chunk = CHUNK // TILE
    scale = LOG2E * inv_lsq
    my_sys = lax.axis_index('sys')
    me = lax.axis_index('seg')
    core = lax.rem(me, 2)
    xc = lax.rem(me // 2, 2)
    yc = me // 4

    def dev(y, x, c):
        return (y * 2 + x) * 2 + c

    owner = {0: me, 1: dev(yc, xc, 1 - core), 2: dev(yc, 1 - xc, core), 3: dev(yc, 1 - xc, 1 - core),
             4: dev(1 - yc, xc, 1 - core), 5: dev(1 - yc, 1 - xc, core), 6: dev(1 - yc, 1 - xc, 1 - core)}
    target = {'core': owner[1], 'x': owner[2], 'yo': owner[4], 'y': dev(1 - yc, xc, core)}

    barrier = pltpu.get_barrier_semaphore()
    for step in range(1, 8):
        pl.semaphore_signal(barrier, inc=1, device_id=(my_sys, lax.rem(me + step, 8)), device_id_type=MESH)

    def loads(c):
        cols = slice(c * CHUNK, (c + 1) * CHUNK)
        return (pltpu.make_async_copy(x_ref.at[:, cols], xj.at[c, pl.ds(0, feat), :], load_x.at[c]),
                pltpu.make_async_copy(q_ref.at[:, cols], qj.at[c], load_q.at[c]))

    band_load = pltpu.make_async_copy(band_ref, band, load_b)
    for c in range(PARTS):
        for copy in loads(c):
            copy.start()
    band_load.start()

    def copies(k):
        src, link, dst = SENDS[k]
        s, d = POS[src], POS[dst]
        to = (my_sys, target[link])
        return (
            pltpu.make_async_remote_copy(src_ref=qj.at[s], dst_ref=qj.at[d], send_sem=send_q.at[k],
                                         recv_sem=recv_q.at[d], device_id=to, device_id_type=MESH),
            pltpu.make_async_remote_copy(src_ref=xj.at[s], dst_ref=xj.at[d], send_sem=send_x.at[k],
                                         recv_sem=recv_x.at[d], device_id=to, device_id_type=MESH))

    def arrived(p):
        to = (my_sys, me)
        pltpu.make_async_remote_copy(src_ref=qj.at[p], dst_ref=qj.at[p], send_sem=send_q.at[0],
                                     recv_sem=recv_q.at[p], device_id=to, device_id_type=MESH).wait_recv()
        pltpu.make_async_remote_copy(src_ref=xj.at[p], dst_ref=xj.at[p], send_sem=send_x.at[0],
                                     recv_sem=recv_x.at[p], device_id=to, device_id_type=MESH).wait_recv()

    row8 = lax.broadcasted_iota(jnp.int32, (8, CHUNK), 0)
    extra_i = []
    for c in range(PARTS):
        cols = slice(c * CHUNK, (c + 1) * CHUNK)
        for copy in loads(c):
            copy.wait()
        x_f = xj[c, 0:feat, :].astype(jnp.float32)
        pieces = split3(-0.5 * jnp.sum(x_f * x_f, axis=0, keepdims=True))
        v_j = jnp.where((row8 >= 3) & (row8 < 6), 1.0, 0.0)
        v_i = jnp.where(row8 < 3, 1.0, 0.0)
        for k in range(3):
            v_j = jnp.where(row8 == k, pieces[k], v_j)
            v_i = jnp.where(row8 == 3 + k, pieces[k], v_i)
        xj[c, feat:depth, :] = v_j.astype(jnp.bfloat16)
        aux[:, cols] = v_i

    band_load.wait()
    pl.semaphore_wait(barrier, 7)
    for k in range(len(FIRSTS)):
        for copy in copies(k):
            copy.start()

    for g in range(n_rows // 128):
        rows = slice(g * 128, (g + 1) * 128)
        c, l0 = g * 128 // CHUNK, g * 128 % CHUNK
        cols = slice(l0, l0 + 128)
        xi[rows, 0:128] = xj[c, 0:128, cols].T
        xi[rows, 128:256] = xj[c, 128:256, cols].T
        last = jnp.concatenate([xj[c, 256:feat, cols].astype(jnp.float32), aux[:, rows],
                                jnp.zeros((384 - depth, 128), jnp.float32)], axis=0)
        xi[rows, 256:384] = last.T.astype(jnp.bfloat16)
        qi[rows, :] = jnp.broadcast_to(qj[c, :, cols], (128, 128)).T

    tr = lax.broadcasted_iota(jnp.int32, (TILE, TILE), 0)
    tc = lax.broadcasted_iota(jnp.int32, (TILE, TILE), 1)
    diag[...] = jnp.where(tr == tc, -1e30, 0.0)
    for ref in (rs, cs_own, eacc):
        ref[...] = jnp.zeros_like(ref)
    for p, (role, _) in enumerate(ORDER):
        mpos[p] = band[0, lax.rem(owner[role] - me + 11, 8)].astype(jnp.float32)

    on_core = core.astype(jnp.float32)
    share = {3: 1.0 - on_core, 4: on_core}
    for p, (role, _) in enumerate(ORDER):
        epos[p] = share.get(role, 0.5 * jnp.ones_like(on_core))

    half = n_tiles // 2
    own_steps = []
    for r in (1, 2, 3):
        a2 = 4 // (r + 1)
        own_steps.append([([2 * a, 2 * a + 1], b, b * CHUNK) for a, b in ((0, r), (a2, 6 - r - a2))])
    own_diag = [([2 * c, 2 * c + 1], c, None) for c in range(PARTS)]
    peer_steps = []
    for k in range(4):
        part = lax.rem(k // 2 + core, 2) * 2 + k % 2
        tiles = list(range(k // 2 * half, (k // 2 + 1) * half))
        peer_steps.append([(tiles, PARTS + part, pl.multiple_of(part * CHUNK, CHUNK))])

    def whole(p):
        return [(list(range(n_tiles)), p, None)]

    def crosses(step, s_new):
        def one(n, t, p, jt):
            rows, cols = slice(t * TILE, (t + 1) * TILE), slice(jt * TILE, (jt + 1) * TILE)
            s_new[n] = jnp.dot(xi[rows, 0:depth], xj[p, :, cols], preferred_element_type=jnp.float32)
        todo = [(t, p, jt) for tiles, p, _ in step for t in tiles for jt in range(per_chunk)]
        return [functools.partial(one, n, *args) for n, args in enumerate(todo)]

    def consume(step, s_old, masked=False, back=None, cs=None, weight=None, fresh=False, back_fresh=False, cs_fresh=False):
        n = 0
        for tiles, p, first in step:
            mark = mpos[p]
            pulls, sums = [None] * per_chunk, [None] * per_chunk
            e_part = jnp.zeros((8, 128), jnp.float32)
            for ti, t in enumerate(tiles):
                rows = slice(t * TILE, (t + 1) * TILE)
                t_lane = t * TILE % CHUNK
                row_part, pull = None, None
                for jt in range(per_chunk):
                    yield
                    cols = slice(jt * TILE, (jt + 1) * TILE)
                    top = diag[...] if masked and ti == jt else 0.0
                    e = jnp.exp2(jnp.minimum(s_old[n], top) * scale)
                    q_rows = qi[rows, :]
                    w = jnp.concatenate([e[:, 0:128] * q_rows, e[:, 128:256] * q_rows], axis=1)
                    w = w * (qj[p, :, cols] * mark)
                    part = w[:, 0:128] + w[:, 128:256]
                    row_part = part if row_part is None else row_part + part
                    w_low = w.astype(jnp.bfloat16)
                    prod = lax.dot_general(xj[p, 0:feat, cols], w_low, (((1,), (1,)), ((), ())),
                                           preferred_element_type=jnp.float32)
                    pull = prod if pull is None else pull + prod
                    if back is not None:
                        prod = jnp.dot(xj[t * TILE // CHUNK, 0:feat, t_lane:t_lane + TILE], w_low,
                                       preferred_element_type=jnp.float32)
                        pulls[jt] = prod if pulls[jt] is None else pulls[jt] + prod
                        part = jnp.sum(w.reshape(TILE // 8, 8, TILE), axis=0)
                        sums[jt] = part if sums[jt] is None else sums[jt] + part
                    n += 1
                acc[:, rows] = pull if fresh else acc[:, rows] + pull
                rs[rows, :] += row_part
                e_part = e_part + jnp.sum(row_part.reshape(TILE // 8, 8, 128), axis=0)
            eacc[...] += e_part * (epos[p] if weight is None else weight)
            if back is not None:
                for jt in range(per_chunk):
                    cols = pl.ds(first + jt * TILE, TILE)
                    back[:, cols] = pulls[jt] if back_fresh else back[:, cols] + pulls[jt]
                    cs[:, cols] = sums[jt] if cs_fresh else cs[:, cols] + sums[jt]

    def phase(new, eaten, n_eaten):
        given = 0
        for k, _ in enumerate(eaten):
            upto = -(-len(new) * (k + 1) // n_eaten)
            for f in new[given:upto]:
                f()
            given = max(given, upto)

    for f in crosses(own_steps[0], s1):
        f()
    own = dict(back=acc, cs=cs_own, weight=1.0)
    peer = dict(back=react, cs=cs_react, weight=1.0, back_fresh=True, cs_fresh=True)
    phase(crosses(own_steps[1], s0), consume(own_steps[0], s1, fresh=True, back_fresh=True, **own), 8)
    phase(crosses(own_steps[2], s1), consume(own_steps[1], s0, **own), 8)
    phase(crosses(own_diag, s0), consume(own_steps[2], s1, **own), 8)
    for c in range(PARTS):
        arrived(PARTS + c)
    phase(crosses(peer_steps[0], s1), consume(own_diag, s0, masked=True, weight=0.5), 16)
    phase(crosses(peer_steps[1], s0), consume(peer_steps[0], s1, **peer), 8)
    phase(crosses(peer_steps[2], s1), consume(peer_steps[1], s0, **peer), 8)

    def pass_on(p):
        for k in range(len(FIRSTS), len(FIRSTS) + len(FORWARDS)):
            if POS[SENDS[k][0]] == p:
                for copy in copies(k):
                    copy.start()

    for p in (2 * PARTS, 2 * PARTS + 1):
        arrived(p)
        pass_on(p)
    phase(crosses(peer_steps[3], s0), consume(peer_steps[2], s1, **peer), 8)
    phase(crosses(whole(2 * PARTS), s1), consume(peer_steps[3], s0, **peer), 8)

    def gifts():
        to = (my_sys, owner[1])
        return (
            pltpu.make_async_remote_copy(src_ref=react, dst_ref=gift, send_sem=send_g.at[0],
                                         recv_sem=recv_g.at[0], device_id=to, device_id_type=MESH),
            pltpu.make_async_remote_copy(src_ref=cs_react, dst_ref=cs_gift, send_sem=send_g.at[1],
                                         recv_sem=recv_g.at[1], device_id=to, device_id_type=MESH))

    forward_at = sorted({POS[f[0]] for f in FORWARDS})

    n_pairs = (N_CHUNK - 2 * PARTS - 4) // 2

    def pair(i, carry):
        p1, p2 = 2 * i + 2 * PARTS + 1, 2 * i + 2 * PARTS + 2

        @pl.when(i > 0)
        def _():
            arrived(p1)

        arrived(p2)
        for f in range(n_pairs):
            due = [fp for fp in forward_at if fp - 2 * PARTS in (2 * f + 1, 2 * f + 2) and fp > 2 * PARTS + 1]
            if due or f == 1:
                @pl.when(i == f)
                def _():
                    for fp in due:
                        pass_on(fp)
                    if f == 1:
                        for k in range(len(FIRSTS) + len(FORWARDS), len(SENDS)):
                            for copy in copies(k):
                                copy.start()
                        for copy in gifts():
                            copy.start()

        phase(crosses(whole(p1), s0), consume(whole(p1 - 1), s1), 16)
        phase(crosses(whole(p2), s1), consume(whole(p1), s0), 16)
        return carry

    lax.fori_loop(0, n_pairs, pair, 0)
    p_late, p_end = N_CHUNK - 1 - core, N_CHUNK - 2 + core
    arrived(N_CHUNK - 3)
    pass_on(N_CHUNK - 3)
    phase(crosses(whole(N_CHUNK - 3), s0), consume(whole(N_CHUNK - 4), s1), 16)
    arrived(N_CHUNK - 2)
    arrived(N_CHUNK - 1)
    for copy in gifts():
        copy.wait_recv()
    phase(crosses(whole(p_late), s1), consume(whole(N_CHUNK - 3), s0), 16)
    phase(crosses(whole(p_end), s0), consume(whole(p_late), s1), 16)
    eslot[me] = eacc[...]

    def finish(t):
        for r0 in (t * TILE, t * TILE + 128):
            rows = slice(r0, r0 + 128)
            c, l0 = r0 // CHUNK, r0 % CHUNK
            total = jnp.sum(rs[rows, :].T, axis=0, keepdims=True)
            total = total + jnp.sum(cs_own[:, rows] + cs_gift[:, rows], axis=0, keepdims=True)
            x_part = xj[c, 0:feat, l0:l0 + 128].astype(jnp.float32)
            out_ref[:, rows] = (total * x_part - (acc[:, rows] + gift[:, rows])) * inv_lsq

    def energy_copy(step):
        return pltpu.make_async_remote_copy(
            src_ref=eslot.at[me], dst_ref=eslot.at[me], send_sem=send_e.at[step - 1],
            recv_sem=recv_e.at[step - 1], device_id=(my_sys, lax.rem(me + step, 8)), device_id_type=MESH)

    for n, _ in enumerate(consume(whole(p_end), s0)):
        if n == 2:
            for step in range(1, 8):
                energy_copy(step).start()
        if n and n % 2 == 0:
            finish(n // 2 - 1)
    finish(n_tiles - 1)
    for k in range(len(SENDS)):
        for copy in copies(k):
            copy.wait_send()
    for copy in gifts():
        copy.wait_send()
    for step in range(1, 8):
        energy_copy(step).wait_send()
        src = lax.rem(me - step + 8, 8)
        pltpu.make_async_remote_copy(
            src_ref=eslot.at[src], dst_ref=eslot.at[src], send_sem=send_e.at[step - 1],
            recv_sem=recv_e.at[step - 1], device_id=(my_sys, me), device_id_type=MESH).wait_recv()
    total = eslot[0]
    for d in range(1, 8):
        total = total + eslot[d]
    en_ref[0] = jnp.sum(total)


def solution(mesh):
    def device_fn(positions, charges, pair_band):
        n_rows, feat = positions.shape
        depth = feat + 8
        vmem = pl.BlockSpec(memory_space=pltpu.VMEM)
        hbm = pl.BlockSpec(memory_space=pltpu.HBM)
        f32, bf16 = jnp.float32, jnp.bfloat16
        dma = pltpu.SemaphoreType.DMA
        forces, energy = pl.pallas_call(
            functools.partial(kernel, 1.0 / feat),
            out_shape=[pltpu.VMEM((feat, n_rows), f32), jax.ShapeDtypeStruct((1,), f32)],
            in_specs=[hbm, hbm, hbm],
            out_specs=[vmem, pl.BlockSpec(memory_space=pltpu.SMEM)],
            scratch_shapes=[
                pltpu.VMEM((n_rows, 384), bf16),
                pltpu.VMEM((N_CHUNK, depth, CHUNK), bf16),
                pltpu.VMEM((N_CHUNK, 1, CHUNK), f32),
                pltpu.VMEM((n_rows, 128), f32),
                pltpu.VMEM((n_rows // 128, TILE, TILE), f32),
                pltpu.VMEM((n_rows // 128, TILE, TILE), f32),
                pltpu.VMEM((feat, n_rows), f32),
                pltpu.VMEM((feat, n_rows), f32),
                pltpu.VMEM((feat, n_rows), f32),
                pltpu.VMEM((n_rows, 128), f32),
                pltpu.VMEM((8, n_rows), f32),
                pltpu.VMEM((8, n_rows), f32),
                pltpu.VMEM((8, n_rows), f32),
                pltpu.VMEM((TILE, TILE), f32),
                pltpu.VMEM((8, 8, 128), f32),
                pltpu.VMEM((8, 128), f32),
                pltpu.SMEM(pair_band.shape, jnp.int32),
                pltpu.SMEM((N_CHUNK,), f32),
                pltpu.SMEM((N_CHUNK,), f32),
                pltpu.VMEM((8, n_rows), f32),
                dma((len(SENDS),)), dma((N_CHUNK,)), dma((len(SENDS),)), dma((N_CHUNK,)),
                dma((7,)), dma((7,)), dma((2,)), dma((2,)), dma((PARTS,)), dma((PARTS,)), dma,
            ],
            compiler_params=pltpu.CompilerParams(
                collective_id=0, has_side_effects=True, vmem_limit_bytes=64421888),
            name='pair_forces',
        )(positions.T, charges.reshape(1, n_rows), pair_band)
        return forces.T, energy

    row_spec = P(('sys', 'seg'), None)
    vec_spec = P(('sys', 'seg'))
    return jax.shard_map(device_fn, mesh=mesh, in_specs=(row_spec, vec_spec, row_spec),
                         out_specs=(row_spec, P('sys')), check_vma=False)
```
